32 devices in a mesh: ctx: 16 (over z, x, core), wt: 2 (over y).
Axes of the slice: x: 2, y: 2, z: 4, core: 2. Of those that a mesh axis runs over, the one named last changes fastest.
Arguments:
- patches: bfloat16 [8192, 1280], P('ctx'), may hold values from -6 to 6
- vit_gain: float32 [1280], replicated, may hold values from 0.5 to 1.5
- vit_codes: bfloat16 [1280, 3, 1280], P(None, None, 'wt'), may hold values from -1 to 1
- vit_scales: bfloat16 [2], P('wt'), may hold values from 0.5 to 2
- vit_bias: float32 [3, 1280], P(None, 'wt'), may hold values from -3 to 3
- window_ids: int32 [8192], P('ctx'), may hold values from 63 to 8191, as said below
- merger_codes: bfloat16 [4, 1280, 8192], P(None, 'wt', 'ctx'), may hold values from -0.078125 to 0.078125
- merger_scales: bfloat16 [1, 2, 8192], P(None, 'wt', 'ctx'), may hold values from 0.5 to 2
- merger_bias: float32 [8192], P('wt'), may hold values from -3 to 3
- positions: int32 [2048], P('ctx'), may hold values from 0 to 8191, as said below
- text_embed: bfloat16 [8192, 8192], P('ctx', 'wt'), may hold values from -6 to 6
- norm_gain: float32 [8192], P('wt'), may hold values from 0.5 to 1.5
- llm_codes: bfloat16 [8192, 8, 768], P('wt', None, 'ctx'), may hold values from -1 to 1
- llm_scales: bfloat16 [2, 8, 768], P('wt', None, 'ctx'), may hold values from 0.5 to 2
- llm_bias: float32 [8, 768], P('wt'), may hold values from -3 to 3
- segments: int32 [8192], P('ctx'), may hold values from 0 to 7, never falling along the last dimension, each value on 1 to 2048 neighbouring positions
Outputs:
- attention_out: bfloat16 [8192, 4096], P('ctx', 'wt')
The draws below stay inside these ranges and needn't reach their ends.
Inputs may be any that keep to these rules, and one draw needn't show every extreme that they name: `window_ids`: windows are runs of consecutive patches of at most 64, never crossing a block of 512 patches; patches of one window share the id, different windows have different ids. `positions`: distinct. The 128 entries of one aligned block (one device's merged tokens) put at most 16 into any one block of 512 positions, and exactly 16 into some block. `segments`: never falling; each run of equal ids is at most 2048 positions long.
All inputs are finite; a program needn't handle non-finite values.
Results may differ from the reference program's by a relative error of at most 0.025.
Values may be sent and summed in bfloat16 or wider, within the bound.
No kernel may reach another device: no remote copies, remote signals or barrier semaphores. Data moves between devices by JAX's collectives and lax.ppermute only.
A program may use at most 192 MiB of HBM per device.

```python
import math
import jax
import jax.numpy as jnp
import numpy as np
from jax import lax

VD = 1280
VHD = 80
D = 8192
KVH = 8
HD = 128
GROUP = 4
MERGE = 4
WIN = 64
REACH = 4
P_DEV = 512
C_DEV = 512
IMG_DEV = 128
CAP = 16
PATCHES = 8192
IMG_TOKENS = 2048
TOKENS = 8192
GW = 768
N_CTX = 16
N_WT = 2


def draw_window_ids(key, part):
    shards = PATCHES // P_DEV
    pieces = P_DEV // 4 + 1
    lengths = 4 * jax.random.randint(key, (shards, pieces), 1, WIN // 4 + 1)
    lengths = lengths.at[:, 0].set(WIN)
    end_index = jnp.cumsum(lengths, axis=1)
    patch_index = jnp.arange(P_DEV)
    local = jnp.sum((end_index[:, None, :] <= patch_index[None, :, None]).astype(jnp.int32), axis=2)
    window_end = jnp.take_along_axis(end_index, local, axis=1)
    window_end = jnp.minimum(window_end, P_DEV)
    labels = window_end - 1 + jnp.arange(shards)[:, None] * P_DEV
    return labels.reshape(-1).astype(jnp.int32)


def draw_positions(key, part):
    owners = TOKENS // C_DEV
    group_size = C_DEV // owners
    source_keys = jax.random.split(key, owners)

    def one_source(source_key, source):
        perm_key, lift_key, start_key = jax.random.split(source_key, 3)
        owner_order = jax.random.permutation(perm_key, owners)
        lift_sizes = jax.random.randint(lift_key, (owners // 2,), 0, CAP // 2 + 1)
        lift_sizes = lift_sizes.at[0].set(CAP // 2)
        paired = jnp.stack([CAP // 2 + lift_sizes, CAP // 2 - lift_sizes], axis=1).reshape(-1)
        counts = jnp.zeros((owners,), jnp.int32).at[owner_order].set(paired.astype(jnp.int32))
        starts = jax.random.randint(start_key, (owners,), 0, group_size - counts + 1)
        end_index = jnp.cumsum(counts)
        token_index = jnp.arange(IMG_DEV)
        target = jnp.sum((end_index[None, :] <= token_index[:, None]).astype(jnp.int32), axis=1)
        begin_index = end_index[target] - counts[target]
        return target * C_DEV + source * group_size + starts[target] + token_index - begin_index
    placed = jax.vmap(one_source)(source_keys, jnp.arange(owners))
    return placed.reshape(-1).astype(jnp.int32)


def loguniform_draw(base_key, shape):
    drawn = jax.random.uniform(base_key, shape, jnp.float32, math.log(0.5), math.log(2.0))
    return jnp.exp(drawn)


def draw_patches(key, part):
    noise = jnp.clip(jax.random.normal(jax.random.fold_in(key, 11), (PATCHES, VD), jnp.float32), -6.0, 6.0)
    return jnp.clip(noise, -6.0, 6.0).astype(jnp.bfloat16)


def draw_vit_codes(key, part):
    codes = jnp.clip(jax.random.normal(jax.random.fold_in(key, 21), (VD, 3, VD), jnp.float32), -6.0, 6.0) * VD ** (-0.5)
    return jnp.clip(codes, -1.0, 1.0).astype(jnp.bfloat16)


def draw_vit_scales(key, part):
    scales = loguniform_draw(jax.random.fold_in(key, 31), (N_WT,))
    return scales.astype(jnp.bfloat16)


def draw_text_embed(key, part):
    noise = jnp.clip(jax.random.normal(jax.random.fold_in(key, 41), (TOKENS, D), jnp.float32), -6.0, 6.0)
    return jnp.clip(noise, -6.0, 6.0).astype(jnp.bfloat16)


def draw_llm_codes(key, part):
    codes = jnp.clip(jax.random.normal(jax.random.fold_in(key, 51), (D, KVH, GW), jnp.float32), -6.0, 6.0) * D ** (-0.5)
    return jnp.clip(codes, -1.0, 1.0).astype(jnp.bfloat16)


def draw_llm_scales(key, part):
    scales = loguniform_draw(jax.random.fold_in(key, 61), (N_WT, KVH, GW))
    return scales.astype(jnp.bfloat16)


def steps_of(key, extent, cuts, low, high):
    loudness = 1.0
    for axis_at, parts in cuts:
        heights = jax.random.uniform(jax.random.fold_in(jax.random.fold_in(key, 6), axis_at), (parts,), jnp.float32, low / len(cuts), high / len(cuts))
        loudness = loudness * jnp.repeat(jnp.exp(heights), extent[axis_at] // parts).reshape((-1,) + (1,) * (len(extent) - 1 - axis_at))
    return loudness


def split_up(count, total, reach, slope):
    portions = [(1 << 20) // math.isqrt(standing ** slope) + 1 for standing in range(2, count + 1)]
    spare, holding = total - reach - (count - 1), [1] * (count - 1)
    while spare > 0:
        candidates = [i for i in range(count - 1) if holding[i] < reach]
        whole, left = sum([portions[i] for i in candidates]), spare
        for i in candidates:
            extra = min(reach - holding[i], max(1, left * portions[i] // whole), spare)
            holding[i] = holding[i] + extra
            spare = spare - extra
    return np.array([reach] + holding)


def ragged(key, number_of, total, limit, lean):
    if number_of == 2:
        one = jax.random.randint(key, (), max(1, total - limit), min(limit, total - 1) + 1)
        return jnp.stack([one, total - one])
    sizes = jnp.asarray(split_up(number_of, total, limit, lean), jnp.int32)
    couples = (number_of - 1) // 2
    source_of, sink = sizes[1:1 + 2 * couples:2], sizes[2:2 + 2 * couples:2]
    slack = jnp.minimum(source_of - 1, limit - sink)
    moved = jax.random.randint(jax.random.fold_in(key, 1), (couples,), 0, 1 << 20) % (slack + 1)
    sizes = sizes.at[1:1 + 2 * couples:2].set(source_of - moved).at[2:2 + 2 * couples:2].set(sink + moved)
    return sizes[jax.random.permutation(jax.random.fold_in(key, 2), number_of)]


def bell_draw(own_key, dims, spread, most, cuts=(), kind=jnp.bfloat16):
    values = jax.random.normal(own_key, dims, jnp.float32) * spread
    if len(cuts) > 0:
        values = steps_of(own_key, dims, cuts, -0.22, 0.18) * values
    return jnp.clip(values, min=-most, max=most).astype(kind)


def setup_inputs(seed: int = 0) -> dict:
    key_list = jax.random.split(jax.random.key(seed), 17)
    return {
        "patches": draw_patches(jax.random.fold_in(key_list[16], 71), 0),
        "vit_gain": jnp.clip(1.0 + 0.1 * jax.random.normal(key_list[1], (VD,), jnp.float32), 0.5, 1.5),
        "vit_codes": draw_vit_codes(jax.random.fold_in(key_list[16], 71), 0),
        "vit_scales": draw_vit_scales(jax.random.fold_in(key_list[16], 71), 0),
        "vit_bias": bell_draw(key_list[4], (3, VD), 0.5, 3.0, ((1, 2),), jnp.float32),
        "window_ids": draw_window_ids(jax.random.fold_in(key_list[16], 71), 0),
        "merger_codes": bell_draw(key_list[6], (MERGE, VD, D), (MERGE * VD) ** -0.5, 0.078125, ((1, 2), (2, 16))),
        "merger_scales": jnp.clip(jnp.exp(math.log(2.0) - 1.3862944 * jax.random.uniform(key_list[7], (1, N_WT, D), jnp.float32) ** steps_of(key_list[7], (1, N_WT, D), ((1, 2), (2, 16)), -0.2, 0.2)), 0.5, 2.0).astype(jnp.bfloat16),
        "merger_bias": bell_draw(key_list[8], (D,), 0.5, 3.0, ((0, 2),), jnp.float32),
        "positions": draw_positions(jax.random.fold_in(key_list[16], 71), 0),
        "text_embed": draw_text_embed(jax.random.fold_in(key_list[16], 71), 0),
        "norm_gain": jnp.clip(1.0 + 0.1 * jax.random.normal(key_list[11], (D,), jnp.float32), 0.5, 1.5),
        "llm_codes": draw_llm_codes(jax.random.fold_in(key_list[16], 71), 0),
        "llm_scales": draw_llm_scales(jax.random.fold_in(key_list[16], 71), 0),
        "llm_bias": bell_draw(key_list[14], (KVH, GW), 0.5, 3.0, ((0, 2),), jnp.float32),
        "segments": jnp.searchsorted(jnp.cumsum(ragged(key_list[15], TOKENS // (2 * C_DEV), TOKENS, REACH * C_DEV, 1)), jnp.arange(TOKENS), side="right").astype(jnp.int32),
    }


VIT_EPS = 1e-06
RMS_EPS = 1e-06
ROPE_BASE = 1000000.0
FILL_LOW = -1e+30

def softmax_rows(scores, allowed):
    masked = jnp.where(allowed, scores, FILL_LOW)
    highest = lax.optimization_barrier(jnp.max(masked, axis=-1, keepdims=True))
    raised = jnp.exp(masked - highest)
    return raised / lax.optimization_barrier(jnp.sum(raised, axis=-1, keepdims=True))

def vision_norm_rows(patches, vit_gain):
    values = patches.astype(jnp.float32)
    mean_square = lax.optimization_barrier(jnp.mean(values * values, axis=1, keepdims=True))
    return (values * lax.rsqrt(mean_square + VIT_EPS) * vit_gain).astype(jnp.bfloat16)

def window_attention(normed, weight_block, bias_block, window_ids):
    row_count = normed.shape[0]
    packed = jnp.dot(normed, weight_block.reshape(normed.shape[1], -1), preferred_element_type=jnp.float32)
    triple = (packed.reshape(row_count, 3, -1) + bias_block).astype(jnp.bfloat16)
    heads_here = triple.shape[2] // VHD
    queries = triple[:, 0].reshape(row_count, heads_here, VHD).astype(jnp.float32)
    keys_here = triple[:, 1].reshape(row_count, heads_here, VHD).astype(jnp.float32)
    values_here = triple[:, 2].reshape(row_count, heads_here, VHD).astype(jnp.float32)
    scores = jnp.einsum('qhd,khd->hqk', queries, keys_here) * VHD ** (-0.5)
    allowed = window_ids[:, None] == window_ids[None, :]
    softmaxed = softmax_rows(scores, allowed[None]).astype(jnp.bfloat16)
    blended = jnp.einsum('hqk,khd->qhd', softmaxed.astype(jnp.float32), values_here)
    return blended.astype(jnp.bfloat16).reshape(row_count, -1)

def rope_tables(first, length):
    places = (first + jnp.arange(length, dtype=jnp.int32)).astype(jnp.float32)
    frequency = ROPE_BASE ** (-jnp.arange(0, HD, 2).astype(jnp.float32) / HD)
    angles = places[:, None] * frequency[None, :]
    angles = jnp.concatenate([angles, angles], axis=1)
    return (jnp.cos(angles), jnp.sin(angles))

def rotary(inputs, cosine, sine):
    halfway = inputs.shape[-1] // 2
    turned = jnp.concatenate([-inputs[..., halfway:], inputs[..., :halfway]], axis=-1)
    return inputs * cosine + turned * sine

def split_heads(triple, cosine, sine):
    row_count, group_count = (triple.shape[0], triple.shape[1])
    queries = triple[:, :, :GROUP * HD].reshape(row_count, group_count, GROUP, HD)
    queries = rotary(queries, cosine[:, None, None, :], sine[:, None, None, :]).astype(jnp.bfloat16)
    keys_rot = rotary(triple[:, :, GROUP * HD:(GROUP + 1) * HD], cosine[:, None, :], sine[:, None, :]).astype(jnp.bfloat16)
    values_cut = triple[:, :, (GROUP + 1) * HD:].astype(jnp.bfloat16)
    return (queries, keys_rot, values_cut)

def reference(patches, vit_gain, vit_codes, vit_scales, vit_bias, window_ids, merger_codes, merger_scales, merger_bias, positions, text_embed, norm_gain, llm_codes, llm_scales, llm_bias, segments):
    vit_cols = vit_codes.shape[2] // N_WT
    vit_weight = (vit_codes.astype(jnp.float32) * jnp.repeat(vit_scales.astype(jnp.float32), vit_cols)).astype(jnp.bfloat16)
    normed_patches = vision_norm_rows(patches, vit_gain)
    patch_blocks = normed_patches.reshape(N_CTX, P_DEV, VD)
    window_blocks = window_ids.reshape(N_CTX, P_DEV)
    attended = lax.map(lambda pair: window_attention(pair[0], vit_weight, vit_bias, pair[1]), (patch_blocks, window_blocks))
    attended = attended.reshape(IMG_TOKENS, MERGE, N_WT, VD // N_WT)
    merger_weight = (merger_codes.astype(jnp.float32) * jnp.repeat(merger_scales.astype(jnp.float32), VD // N_WT, axis=1)).astype(jnp.bfloat16)
    merger_weight = merger_weight.reshape(MERGE, N_WT, VD // N_WT, D)
    merger_total = jnp.zeros((IMG_TOKENS, D), jnp.float32)
    for shard_index in range(N_WT):
        partial_value = jnp.dot(attended[:, :, shard_index].reshape(IMG_TOKENS, -1), merger_weight[:, shard_index].reshape(-1, D), preferred_element_type=jnp.float32)
        merger_total = merger_total + lax.optimization_barrier(partial_value.astype(jnp.bfloat16)).astype(jnp.float32)
    merged_embed = (merger_total + merger_bias).astype(jnp.bfloat16)
    hidden = text_embed.at[positions].set(merged_embed)
    values = hidden.astype(jnp.float32)
    mean_square = lax.optimization_barrier(jnp.mean(values * values, axis=1, keepdims=True))
    normed = (values * lax.rsqrt(mean_square + RMS_EPS) * norm_gain).astype(jnp.bfloat16)
    rows_wt = D // N_WT
    llm_weight = (llm_codes.astype(jnp.float32) * jnp.repeat(llm_scales.astype(jnp.float32), rows_wt, axis=0)).astype(jnp.bfloat16)
    projected = jnp.zeros((TOKENS, KVH * GW), jnp.float32)
    for shard_index in range(N_WT):
        partial_value = jnp.dot(normed[:, shard_index * rows_wt:(shard_index + 1) * rows_wt], llm_weight[shard_index * rows_wt:(shard_index + 1) * rows_wt].reshape(rows_wt, -1), preferred_element_type=jnp.float32)
        projected = projected + lax.optimization_barrier(partial_value.astype(jnp.bfloat16)).astype(jnp.float32)
    triple = projected.reshape(TOKENS, KVH, GW) + llm_bias
    cosine, sine = rope_tables(0, TOKENS)
    queries, keys_rot, values_cut = split_heads(triple, cosine, sine)
    padding = REACH * C_DEV
    window_len = (REACH + 1) * C_DEV
    keys_pad = jnp.concatenate([jnp.zeros((padding, KVH, HD), jnp.bfloat16), keys_rot], axis=0)
    values_pad = jnp.concatenate([jnp.zeros((padding, KVH, HD), jnp.bfloat16), values_cut], axis=0)
    segments_pad = jnp.concatenate([jnp.zeros((padding,), jnp.int32), segments], axis=0)
    places_pad = jnp.arange(TOKENS + padding, dtype=jnp.int32) - padding

    def attend_block(block_index):
        first_row = (block_index * C_DEV).astype(jnp.int32)
        query_rows = lax.dynamic_slice_in_dim(queries, first_row, C_DEV, 0)
        query_segments = lax.dynamic_slice_in_dim(segments, first_row, C_DEV, 0)
        key_rows = lax.dynamic_slice_in_dim(keys_pad, first_row, window_len, 0)
        value_rows = lax.dynamic_slice_in_dim(values_pad, first_row, window_len, 0)
        key_segments = lax.dynamic_slice_in_dim(segments_pad, first_row, window_len, 0)
        key_places = lax.dynamic_slice_in_dim(places_pad, first_row, window_len, 0)
        query_places = first_row + jnp.arange(C_DEV, dtype=jnp.int32)
        allowed = (query_segments[:, None] == key_segments[None, :]) & (key_places[None, :] <= query_places[:, None]) & (key_places[None, :] >= 0)
        scores = jnp.einsum('qgjd,kgd->gjqk', query_rows.astype(jnp.float32), key_rows.astype(jnp.float32)) * HD ** (-0.5)
        softmaxed = softmax_rows(scores, allowed[None, None]).astype(jnp.bfloat16)
        blended = jnp.einsum('gjqk,kgd->qgjd', softmaxed.astype(jnp.float32), value_rows.astype(jnp.float32))
        return blended.astype(jnp.bfloat16).reshape(C_DEV, -1)
    result = lax.map(attend_block, jnp.arange(N_CTX, dtype=jnp.int32))
    return result.reshape(TOKENS, -1)
```

```python
import functools
import math

import jax
import jax.numpy as jnp
from jax import lax
from jax.experimental import pallas as pl
from jax.experimental.pallas import tpu as pltpu
from jax.sharding import PartitionSpec as P


VHD = 80
D = 8192
KVH = 8
HD = 128
GROUP = 4
REACH = 4


VIT_EPS = 1e-06
RMS_EPS = 1e-06
ROPE_BASE = 1000000.0
FILL_LOW = -1e30


def shifted(value, axis, steps):
    count = lax.axis_size(axis)
    return lax.ppermute(value, axis, [(i, (i + steps) % count) for i in range(count)])


def passed_along(value, axis, steps):
    count = lax.axis_size(axis)
    return lax.ppermute(value, axis, [(i, i + steps) for i in range(count - steps)])


def softmax_rows(scores, allowed):
    masked = jnp.where(allowed, scores, FILL_LOW)
    highest = jnp.max(masked, axis=-1, keepdims=True)
    raised = jnp.exp(masked - highest)
    return raised / jnp.sum(raised, axis=-1, keepdims=True)


def vision_norm_rows(patches, vit_gain):
    values = patches.astype(jnp.float32)
    mean_square = jnp.mean(values * values, axis=1, keepdims=True)
    return (values * lax.rsqrt(mean_square + VIT_EPS) * vit_gain).astype(jnp.bfloat16)


def window_attention(normed, weight_block, bias_block, window_ids):
    row_count = normed.shape[0]
    packed = jnp.dot(
        normed, weight_block.reshape(normed.shape[1], -1), preferred_element_type=jnp.float32
    )
    triple = (packed.reshape(row_count, 3, -1) + bias_block).astype(jnp.bfloat16)
    heads_here = triple.shape[2] // VHD
    queries = triple[:, 0].reshape(row_count, heads_here, VHD)
    keys_here = triple[:, 1].reshape(row_count, heads_here, VHD)
    values_here = triple[:, 2].reshape(row_count, heads_here, VHD)
    scores = jnp.einsum(
        "qhd,khd->hqk", queries, keys_here, preferred_element_type=jnp.float32
    ) * VHD ** (-0.5)
    allowed = window_ids[:, None] == window_ids[None, :]
    softmaxed = softmax_rows(scores, allowed[None]).astype(jnp.bfloat16)
    blended = jnp.einsum("hqk,khd->qhd", softmaxed, values_here, preferred_element_type=jnp.float32)
    return blended.astype(jnp.bfloat16).reshape(row_count, -1)


def rope_tables(first, length):
    places = (first + jnp.arange(length, dtype=jnp.int32)).astype(jnp.float32)
    frequency = ROPE_BASE ** (-jnp.arange(0, HD, 2).astype(jnp.float32) / HD)
    angles = places[:, None] * frequency[None, :]
    angles = jnp.concatenate([angles, angles], axis=1)
    return (jnp.cos(angles), jnp.sin(angles))


def chip_ring(chips):
    return [0] + list(range(1, chips, 2)) + list(range(chips - 2, 0, -2))


def gather_features(features, numbers):
    count = lax.axis_size("ctx")
    chips = count // 2
    ring = jnp.asarray(chip_ring(chips), jnp.int32)
    order = chip_ring(chips)
    where_on = [order.index(chip) for chip in range(chips)]
    me = lax.axis_index("ctx")
    core = me % 2
    spot = jnp.asarray(where_on, jnp.int32)[me // 2]
    pairs = []
    for at in range(chips):
        pairs.append((2 * order[at], 2 * order[(at + 1) % chips]))
        pairs.append((2 * order[at] + 1, 2 * order[(at - 1) % chips] + 1))
    swap = [(i, i ^ 1) for i in range(count)]
    rows = features.shape[0]
    partner = lax.ppermute(features, "ctx", swap)
    moving = jnp.concatenate([features, partner], axis=0)
    found = [(jnp.stack([me, me + 1 - 2 * core]), moving)]
    way = 1 - 2 * core
    small = lax.all_to_all(
        jnp.broadcast_to(numbers[None, :], (count, numbers.shape[0])),
        "ctx",
        split_axis=0,
        concat_axis=0,
        tiled=True,
    )
    for step in range(1, chips // 2 + 1):
        last = step == chips // 2
        sent = moving[:rows] if last else moving
        moving = lax.ppermute(sent, "ctx", pairs)
        other = lax.ppermute(moving, "ctx", swap)
        near = 2 * ring[(spot - way * step) % chips]
        far = 2 * ring[(spot + way * step) % chips]
        if last:
            found.append((jnp.stack([near + core]), moving))
            found.append((jnp.stack([far + 1 - core]), other))
        else:
            found.append((jnp.stack([near + core, near + 1 - core]), moving))
            found.append((jnp.stack([far + 1 - core, far + core]), other))
    return found, small


def summed_over_wt(parts):
    total = parts[0].astype(jnp.float32)
    for steps in range(1, len(parts)):
        arrived = shifted(parts[steps].astype(jnp.bfloat16), "wt", steps)
        total = total + arrived.astype(jnp.float32)
    return total


def turned_by_wt(pieces):
    count = len(pieces)
    here = lax.axis_index("wt")
    return [lax.select_n((here + k) % count, *pieces) for k in range(count)]


def finish_kernel(
    own_ref, arrived_ref, scale_ref, bias_ref, cosine_ref, sine_ref, *out_refs, rotated
):
    total = own_ref[...]
    for k in range(arrived_ref.shape[0]):
        total = total + arrived_ref[k].astype(jnp.float32)
    total = total * scale_ref[...] + bias_ref[...]
    factor = HD ** (-0.5) * math.log2(math.e)
    at = 0
    for out_ref in out_refs:
        for place in range(out_ref.shape[1] // HD):
            part = total[:, at * HD : (at + 1) * HD]
            if at < rotated:
                part = part * cosine_ref[...] + pltpu.roll(part, HD // 2, 1) * sine_ref[...]
            if at < GROUP:
                part = part * factor
            out_ref[:, place * HD : (place + 1) * HD] = part.astype(jnp.bfloat16)
            at += 1


def finish(own, arrived, row_scale, bias, cosine, sine, rotated, widths):
    rows, width = own.shape[0], sum(widths)
    tile = min(rows, 128)
    row = lambda columns: pl.BlockSpec((tile, columns), lambda i: (i, 0))
    return pl.pallas_call(
        functools.partial(finish_kernel, rotated=rotated),
        out_shape=tuple(jax.ShapeDtypeStruct((rows, cut), jnp.bfloat16) for cut in widths),
        grid=(rows // tile,),
        in_specs=[
            row(width),
            pl.BlockSpec((arrived.shape[0], tile, width), lambda i: (0, i, 0)),
            row(1),
            pl.BlockSpec((1, width), lambda i: (0, 0)),
            row(HD),
            row(HD),
        ],
        out_specs=tuple(row(cut) for cut in widths),
        cost_estimate=pl.CostEstimate(
            flops=20 * rows * width, transcendentals=0, bytes_accessed=12 * rows * width
        ),
        name="finish",
    )(own, arrived, row_scale, bias, cosine, sine)


def attend_kernel(need, q_ref, qseg_ref, kseg_ref, kv_ref, *refs, aliased):
    o_ref = refs[aliased]
    m_ref, l_ref, acc_ref, bar_ref, turned_ref = refs[aliased + 1 :]
    blocks, keys, _ = kv_ref.shape
    rows = q_ref.shape[0]

    def one_block(distance, start):
        same = kseg_ref[distance] == qseg_ref[...]
        if start:
            row = lax.broadcasted_iota(jnp.int32, (keys, rows), 1)
            column = lax.broadcasted_iota(jnp.int32, (keys, rows), 0)
            same = same & (column <= row)
        bar_ref[...] = jnp.where(same, 0.0, FILL_LOW)
        turned_ref[...] = jnp.transpose(kv_ref[distance, :, HD:])

        def one_head(head):
            query = q_ref[:, pl.ds(pl.multiple_of(head * HD, HD), HD)]
            scores = (
                lax.dot_general(
                    kv_ref[distance, :, :HD],
                    query,
                    (((1,), (1,)), ((), ())),
                    preferred_element_type=jnp.float32,
                )
                + bar_ref[...]
            )
            highest = jnp.max(scores, axis=0, keepdims=True)
            if not start:
                before = m_ref[head]
                highest = jnp.maximum(before, highest)
                fade = jnp.exp2(before - highest)
            raised = jnp.exp2(scores - highest)
            total = jnp.sum(raised, axis=0, keepdims=True)
            blended = jnp.dot(
                turned_ref[...], raised.astype(jnp.bfloat16), preferred_element_type=jnp.float32
            )
            if not start:
                total = l_ref[head] * fade + total
                blended = acc_ref[head] * fade + blended
            m_ref[head] = highest
            l_ref[head] = total
            acc_ref[head] = blended

        @pl.loop(0, GROUP // 2)
        def _(couple):
            one_head(2 * couple)
            one_head(2 * couple + 1)

    one_block(0, True)

    @pl.loop(1, blocks)
    def _(distance):
        pl.when(need[distance] > 0)(lambda: one_block(distance, False))

    for head in range(GROUP):
        o_ref[:, head * HD : (head + 1) * HD] = jnp.transpose(acc_ref[head] / l_ref[head]).astype(
            o_ref.dtype
        )


def attend(queries, pieces, query_segments, key_segments, need, group, groups, so_far):
    rows, width = queries.shape
    blocks, keys, _ = pieces.shape
    fixed = lambda shape: pl.BlockSpec(shape, lambda i, *_: (0,) * len(shape))
    aliased = 0 if so_far is None else 1
    return pl.pallas_call(
        functools.partial(attend_kernel, aliased=aliased),
        out_shape=jax.ShapeDtypeStruct((rows, width * groups), jnp.bfloat16),
        grid_spec=pltpu.PrefetchScalarGridSpec(
            num_scalar_prefetch=1,
            grid=(1,),
            in_specs=[
                fixed(queries.shape),
                fixed(query_segments.shape),
                fixed(key_segments.shape),
                fixed(pieces.shape),
            ]
            + [pl.BlockSpec(memory_space=pl.ANY)] * aliased,
            out_specs=pl.BlockSpec((rows, width), lambda i, *_: (0, group)),
            scratch_shapes=[
                pltpu.VMEM((GROUP, 1, rows), jnp.float32),
                pltpu.VMEM((GROUP, 1, rows), jnp.float32),
                pltpu.VMEM((GROUP, HD, rows), jnp.float32),
                pltpu.VMEM((keys, rows), jnp.float32),
                pltpu.VMEM((HD, keys), jnp.bfloat16),
            ],
        ),
        input_output_aliases={5: 0} if aliased else {},
        cost_estimate=pl.CostEstimate(
            flops=4 * rows * width * keys * blocks,
            transcendentals=rows * keys * blocks * GROUP,
            bytes_accessed=2 * rows * width * 4,
        ),
        name="attend",
    )(need, queries, query_segments, key_segments, pieces, *([so_far] * aliased))


def on_device(
    patches,
    vit_gain,
    vit_codes,
    vit_scales,
    vit_bias,
    window_ids,
    merger_codes,
    merger_scales,
    merger_bias,
    positions,
    text_embed,
    norm_gain,
    llm_codes,
    llm_scales,
    llm_bias,
    segments,
):
    row_count, local_rows = text_embed.shape
    owners = lax.axis_size("ctx")
    shares = lax.axis_size("wt")
    me = lax.axis_index("ctx")
    first = me * row_count
    groups_here = KVH // shares

    weight = jnp.transpose(llm_codes, (1, 2, 0)).astype(jnp.float32)
    weight = weight * llm_scales[0].astype(jnp.float32)[:, :, None] * norm_gain[None, None, :]
    weight = weight.astype(jnp.bfloat16)
    turned = jnp.stack(
        turned_by_wt([weight[k * groups_here : (k + 1) * groups_here] for k in range(shares)]),
        axis=1,
    )
    normed_patches = vision_norm_rows(patches, vit_gain)
    vit_weight = (vit_codes.astype(jnp.float32) * vit_scales.astype(jnp.float32)[0]).astype(
        jnp.bfloat16
    )
    attended = window_attention(normed_patches, vit_weight, vit_bias, window_ids)
    token_count = positions.shape[0]
    features = attended.reshape(token_count, -1)

    merger_weight = (merger_codes.astype(jnp.float32) * merger_scales.astype(jnp.float32)).astype(
        jnp.bfloat16
    )
    columns = merger_weight.shape[2]
    merger_weight = merger_weight.reshape(-1, columns)
    found, small = gather_features(features, jnp.concatenate([positions, segments]))
    all_positions = small[:, :token_count]
    all_segments = small[:, token_count:]
    early = max(1, groups_here - 1)
    gathered = [lax.all_gather(turned[:early], "ctx", axis=2, tiled=True)]
    sources = jnp.concatenate([source for source, _ in found])
    products = jnp.concatenate(
        [jnp.dot(rows, merger_weight, preferred_element_type=jnp.float32) for _, rows in found],
        axis=0,
    )
    part = columns // shares
    merged = summed_over_wt(
        turned_by_wt([products[:, k * part : (k + 1) * part] for k in range(shares)])
    ).astype(jnp.bfloat16)

    capacity = 2 * token_count // owners
    slots_each = owners * capacity
    target = all_positions // row_count
    item = jnp.arange(token_count, dtype=jnp.int32)
    before = (target[:, None, :] == target[:, :, None]) & (item[None, None, :] < item[None, :, None])
    ranks = jnp.sum(before.astype(jnp.int32), axis=2)
    slots = (
        target * slots_each + jnp.arange(owners, dtype=jnp.int32)[:, None] * capacity + ranks
    )
    slots_found = jnp.take(slots, sources, axis=0).reshape(-1)
    table = slots_found[None, :] == jnp.arange(owners * slots_each, dtype=jnp.int32)[:, None]
    mine = slots.reshape(1, -1) == me * slots_each + jnp.arange(slots_each, dtype=jnp.int32)[:, None]
    labels = jnp.sum(jnp.where(mine, all_positions.reshape(1, -1) + 1, 0), axis=1) - 1 - first
    place = labels[None, :] == jnp.arange(row_count, dtype=jnp.int32)[:, None]
    covered = jnp.any(place, axis=1)[:, None]
    table, place, covered = lax.optimization_barrier(
        (table.astype(jnp.bfloat16), place.astype(jnp.bfloat16), covered.astype(jnp.float32))
    )
    packed = jnp.dot(table, merged, preferred_element_type=jnp.float32).astype(jnp.bfloat16)
    arrived = lax.all_to_all(
        packed.reshape(owners, slots_each, part), "ctx", split_axis=0, concat_axis=0, tiled=True
    )
    if early < groups_here:
        late, arrived = lax.optimization_barrier((turned[early:], arrived))
        gathered.append(lax.all_gather(late, "ctx", axis=2, tiled=True))
    ours = turned_by_wt([block for block in arrived.reshape(shares, -1, slots_each, part)])
    held = [ours[0]] + [shifted(ours[k], "wt", k) for k in range(1, shares)]
    here = lax.axis_index("wt")
    whole_columns = jnp.concatenate(
        [lax.select_n((here - k) % shares, *held) for k in range(shares)], axis=2
    )
    flat = jnp.transpose(whole_columns, (1, 0, 2)).reshape(slots_each, -1)
    filled = jnp.dot(place, flat, preferred_element_type=jnp.float32)
    hidden = lax.optimization_barrier(
        jnp.where(covered > 0, (filled + merger_bias).astype(jnp.bfloat16), text_embed)
    )
    values = hidden.astype(jnp.float32)
    share = jnp.sum(values * values, axis=1)
    squares = share + sum(shifted(share, "wt", k) for k in range(1, shares))
    row_scale = lax.rsqrt(squares[:, None] / D + RMS_EPS)

    cosine, sine = rope_tables(first, row_count)
    sine = jnp.where(jnp.arange(HD) < HD // 2, -sine, sine)
    blocks = REACH + 1
    shards = me - jnp.arange(blocks, dtype=jnp.int32)
    key_segments = jnp.take(all_segments, jnp.maximum(shards, 0), axis=0)
    need = ((shards >= 0) & (key_segments[:, -1] >= segments[0])).astype(jnp.int32)
    query_segments = segments[None, :]
    key_segments = key_segments[:, :, None]
    ends = GROUP * HD
    full = ends + 2 * HD
    output = None
    for group in range(groups_here):
        held_at, at = (gathered[0], group) if group < early else (gathered[1], group - early)

        if group > 0:
            if group < early:
                held_at, product = lax.optimization_barrier((held_at, product))
                gathered[0] = held_at
            else:
                hidden, pieces = lax.optimization_barrier((hidden, pieces))
        if group > 0:
            output = attend(
                queries, pieces, query_segments, key_segments, need, group - 1, groups_here, output
            )
        columns_here = held_at[at].reshape(shares * full, local_rows)
        product = lax.dot_general(
            hidden, columns_here, (((1,), (1,)), ((), ())), preferred_element_type=jnp.float32
        )
        if group == 0:
            product, row_scale = lax.optimization_barrier((product, row_scale))
        arrived = jnp.stack(
            [
                shifted(product[:, k * full : (k + 1) * full].astype(jnp.bfloat16), "wt", k)
                for k in range(1, shares)
            ]
        )
        queries, pair = finish(
            product,
            arrived,
            row_scale,
            llm_bias[group][None, :],
            cosine,
            sine,
            GROUP + 1,
            [ends, 2 * HD],
        )
        pieces = jnp.stack(
            [pair] + [passed_along(pair, "ctx", distance) for distance in range(1, blocks)]
        )
    output = attend(
        queries, pieces, query_segments, key_segments, need, group, groups_here, output
    )
    return output


def solution(mesh):
    in_specs = (
        P("ctx", None),
        P(),
        P(None, None, "wt"),
        P("wt"),
        P(None, "wt"),
        P("ctx"),
        P(None, "wt", "ctx"),
        P(None, "wt", "ctx"),
        P("wt"),
        P("ctx"),
        P("ctx", "wt"),
        P("wt"),
        P("wt", None, "ctx"),
        P("wt", None, "ctx"),
        P("wt", None),
        P("ctx"),
    )
    out_specs = P("ctx", "wt")

    return jax.shard_map(
        on_device, mesh=mesh, in_specs=in_specs, out_specs=out_specs, check_vma=False
    )
```

```python
import functools
import math

import jax
import jax.numpy as jnp
from jax import lax
from jax.experimental import pallas as pl
from jax.experimental.pallas import tpu as pltpu
from jax.sharding import PartitionSpec as P


VHD = 80
D = 8192
KVH = 8
HD = 128
GROUP = 4
REACH = 4


VIT_EPS = 1e-06
RMS_EPS = 1e-06
ROPE_BASE = 1000000.0
FILL_LOW = -1e30


def shifted(value, axis, steps):
    count = lax.axis_size(axis)
    return lax.ppermute(value, axis, [(i, (i + steps) % count) for i in range(count)])


def passed_along(value, axis, steps):
    count = lax.axis_size(axis)
    return lax.ppermute(value, axis, [(i, i + steps) for i in range(count - steps)])


def softmax_rows(scores, allowed):
    masked = jnp.where(allowed, scores, FILL_LOW)
    highest = jnp.max(masked, axis=-1, keepdims=True)
    raised = jnp.exp(masked - highest)
    return raised / jnp.sum(raised, axis=-1, keepdims=True)


def vision_norm_rows(patches, vit_gain):
    values = patches.astype(jnp.float32)
    mean_square = jnp.mean(values * values, axis=1, keepdims=True)
    return (values * lax.rsqrt(mean_square + VIT_EPS) * vit_gain).astype(jnp.bfloat16)


def window_attention(normed, weight_block, bias_block, window_ids):
    row_count = normed.shape[0]
    packed = jnp.dot(
        normed, weight_block.reshape(normed.shape[1], -1), preferred_element_type=jnp.float32
    )
    triple = (packed.reshape(row_count, 3, -1) + bias_block).astype(jnp.bfloat16)
    heads_here = triple.shape[2] // VHD
    queries = triple[:, 0].reshape(row_count, heads_here, VHD)
    keys_here = triple[:, 1].reshape(row_count, heads_here, VHD)
    values_here = triple[:, 2].reshape(row_count, heads_here, VHD)
    scores = jnp.einsum(
        "qhd,khd->hqk", queries, keys_here, preferred_element_type=jnp.float32
    ) * VHD ** (-0.5)
    allowed = window_ids[:, None] == window_ids[None, :]
    softmaxed = softmax_rows(scores, allowed[None]).astype(jnp.bfloat16)
    blended = jnp.einsum("hqk,khd->qhd", softmaxed, values_here, preferred_element_type=jnp.float32)
    return blended.astype(jnp.bfloat16).reshape(row_count, -1)


def rope_tables(first, length):
    places = (first + jnp.arange(length, dtype=jnp.int32)).astype(jnp.float32)
    frequency = ROPE_BASE ** (-jnp.arange(0, HD, 2).astype(jnp.float32) / HD)
    angles = places[:, None] * frequency[None, :]
    angles = jnp.concatenate([angles, angles], axis=1)
    return (jnp.cos(angles), jnp.sin(angles))


def chip_ring(chips):
    return [0] + list(range(1, chips, 2)) + list(range(chips - 2, 0, -2))


def gather_features(features, numbers):
    count = lax.axis_size("ctx")
    chips = count // 2
    ring = jnp.asarray(chip_ring(chips), jnp.int32)
    order = chip_ring(chips)
    where_on = [order.index(chip) for chip in range(chips)]
    me = lax.axis_index("ctx")
    core = me % 2
    spot = jnp.asarray(where_on, jnp.int32)[me // 2]
    pairs = []
    for at in range(chips):
        pairs.append((2 * order[at], 2 * order[(at + 1) % chips]))
        pairs.append((2 * order[at] + 1, 2 * order[(at - 1) % chips] + 1))
    swap = [(i, i ^ 1) for i in range(count)]
    rows = features.shape[0]
    partner = lax.ppermute(features, "ctx", swap)
    moving = jnp.concatenate([features, partner], axis=0)
    found = [(jnp.stack([me, me + 1 - 2 * core]), moving)]
    way = 1 - 2 * core
    small = lax.all_to_all(
        jnp.broadcast_to(numbers[None, :], (count, numbers.shape[0])),
        "ctx",
        split_axis=0,
        concat_axis=0,
        tiled=True,
    )
    for step in range(1, chips // 2 + 1):
        last = step == chips // 2
        sent = moving[:rows] if last else moving
        moving = lax.ppermute(sent, "ctx", pairs)
        other = lax.ppermute(moving, "ctx", swap)
        near = 2 * ring[(spot - way * step) % chips]
        far = 2 * ring[(spot + way * step) % chips]
        if last:
            found.append((jnp.stack([near + core]), moving))
            found.append((jnp.stack([far + 1 - core]), other))
        else:
            found.append((jnp.stack([near + core, near + 1 - core]), moving))
            found.append((jnp.stack([far + 1 - core, far + core]), other))
    return found, small


def summed_over_wt(parts):
    total = parts[0].astype(jnp.float32)
    for steps in range(1, len(parts)):
        arrived = shifted(parts[steps].astype(jnp.bfloat16), "wt", steps)
        total = total + arrived.astype(jnp.float32)
    return total


def turned_by_wt(pieces):
    count = len(pieces)
    here = lax.axis_index("wt")
    return [lax.select_n((here + k) % count, *pieces) for k in range(count)]


def finish_kernel(
    own_ref, arrived_ref, scale_ref, bias_ref, cosine_ref, sine_ref, *out_refs, rotated
):
    total = own_ref[...]
    for k in range(arrived_ref.shape[0]):
        total = total + arrived_ref[k].astype(jnp.float32)
    total = total * scale_ref[...] + bias_ref[...]
    factor = HD ** (-0.5) * math.log2(math.e)
    at = 0
    for out_ref in out_refs:
        for place in range(out_ref.shape[1] // HD):
            part = total[:, at * HD : (at + 1) * HD]
            if at < rotated:
                part = part * cosine_ref[...] + pltpu.roll(part, HD // 2, 1) * sine_ref[...]
            if at < GROUP:
                part = part * factor
            out_ref[:, place * HD : (place + 1) * HD] = part.astype(jnp.bfloat16)
            at += 1


def finish(own, arrived, row_scale, bias, cosine, sine, rotated, widths):
    rows, width = own.shape[0], sum(widths)
    tile = min(rows, 128)
    row = lambda columns: pl.BlockSpec((tile, columns), lambda i: (i, 0))
    return pl.pallas_call(
        functools.partial(finish_kernel, rotated=rotated),
        out_shape=tuple(jax.ShapeDtypeStruct((rows, cut), jnp.bfloat16) for cut in widths),
        grid=(rows // tile,),
        in_specs=[
            row(width),
            pl.BlockSpec((arrived.shape[0], tile, width), lambda i: (0, i, 0)),
            row(1),
            pl.BlockSpec((1, width), lambda i: (0, 0)),
            row(HD),
            row(HD),
        ],
        out_specs=tuple(row(cut) for cut in widths),
        cost_estimate=pl.CostEstimate(
            flops=20 * rows * width, transcendentals=0, bytes_accessed=12 * rows * width
        ),
        name="finish",
    )(own, arrived, row_scale, bias, cosine, sine)


def attend_kernel(need, q_ref, qseg_ref, kseg_ref, kv_ref, *refs, aliased):
    o_ref = refs[aliased]
    m_ref, l_ref, acc_ref, bar_ref, turned_ref = refs[aliased + 1 :]
    blocks, keys, _ = kv_ref.shape
    rows = q_ref.shape[0]

    def one_block(distance, start):
        same = kseg_ref[distance] == qseg_ref[...]
        if start:
            row = lax.broadcasted_iota(jnp.int32, (keys, rows), 1)
            column = lax.broadcasted_iota(jnp.int32, (keys, rows), 0)
            same = same & (column <= row)
        bar_ref[...] = jnp.where(same, 0.0, FILL_LOW)
        turned_ref[...] = jnp.transpose(kv_ref[distance, :, HD:])

        def one_head(head):
            query = q_ref[:, pl.ds(pl.multiple_of(head * HD, HD), HD)]
            scores = (
                lax.dot_general(
                    kv_ref[distance, :, :HD],
                    query,
                    (((1,), (1,)), ((), ())),
                    preferred_element_type=jnp.float32,
                )
                + bar_ref[...]
            )
            highest = jnp.max(scores, axis=0, keepdims=True)
            if not start:
                before = m_ref[head]
                highest = jnp.maximum(before, highest)
                fade = jnp.exp2(before - highest)
            raised = jnp.exp2(scores - highest)
            total = jnp.sum(raised, axis=0, keepdims=True)
            blended = jnp.dot(
                turned_ref[...], raised.astype(jnp.bfloat16), preferred_element_type=jnp.float32
            )
            if not start:
                total = l_ref[head] * fade + total
                blended = acc_ref[head] * fade + blended
            m_ref[head] = highest
            l_ref[head] = total
            acc_ref[head] = blended

        @pl.loop(0, GROUP // 2)
        def _(couple):
            one_head(2 * couple)
            one_head(2 * couple + 1)

    one_block(0, True)

    @pl.loop(1, blocks)
    def _(distance):
        pl.when(need[distance] > 0)(lambda: one_block(distance, False))

    for head in range(GROUP):
        o_ref[:, head * HD : (head + 1) * HD] = jnp.transpose(acc_ref[head] / l_ref[head]).astype(
            o_ref.dtype
        )


def attend(queries, pieces, column, query_segments, key_segments, need, group, groups, so_far):
    rows, width = queries.shape
    blocks, keys, _ = pieces.shape
    fixed = lambda shape: pl.BlockSpec(shape, lambda i, *_: (0,) * len(shape))
    aliased = 0 if so_far is None else 1
    return pl.pallas_call(
        functools.partial(attend_kernel, aliased=aliased),
        out_shape=jax.ShapeDtypeStruct((rows, width * groups), jnp.bfloat16),
        grid_spec=pltpu.PrefetchScalarGridSpec(
            num_scalar_prefetch=1,
            grid=(1,),
            in_specs=[
                fixed(queries.shape),
                fixed(query_segments.shape),
                fixed(key_segments.shape),
                pl.BlockSpec((blocks, keys, 2 * HD), lambda i, *_: (0, 0, column)),
            ]
            + [pl.BlockSpec(memory_space=pl.ANY)] * aliased,
            out_specs=pl.BlockSpec((rows, width), lambda i, *_: (0, group)),
            scratch_shapes=[
                pltpu.VMEM((GROUP, 1, rows), jnp.float32),
                pltpu.VMEM((GROUP, 1, rows), jnp.float32),
                pltpu.VMEM((GROUP, HD, rows), jnp.float32),
                pltpu.VMEM((keys, rows), jnp.float32),
                pltpu.VMEM((HD, keys), jnp.bfloat16),
            ],
        ),
        input_output_aliases={5: 0} if aliased else {},
        cost_estimate=pl.CostEstimate(
            flops=4 * rows * width * keys * blocks,
            transcendentals=rows * keys * blocks * GROUP,
            bytes_accessed=2 * rows * width * 4,
        ),
        name="attend",
    )(need, queries, query_segments, key_segments, pieces, *([so_far] * aliased))


def on_device(
    patches,
    vit_gain,
    vit_codes,
    vit_scales,
    vit_bias,
    window_ids,
    merger_codes,
    merger_scales,
    merger_bias,
    positions,
    text_embed,
    norm_gain,
    llm_codes,
    llm_scales,
    llm_bias,
    segments,
):
    row_count, local_rows = text_embed.shape
    owners = lax.axis_size("ctx")
    shares = lax.axis_size("wt")
    me = lax.axis_index("ctx")
    first = me * row_count
    groups_here = KVH // shares

    weight = jnp.transpose(llm_codes, (1, 2, 0)).astype(jnp.float32)
    weight = weight * llm_scales[0].astype(jnp.float32)[:, :, None] * norm_gain[None, None, :]
    weight = weight.astype(jnp.bfloat16)
    turned = jnp.stack(
        turned_by_wt([weight[k * groups_here : (k + 1) * groups_here] for k in range(shares)]),
        axis=1,
    )
    normed_patches = vision_norm_rows(patches, vit_gain)
    vit_weight = (vit_codes.astype(jnp.float32) * vit_scales.astype(jnp.float32)[0]).astype(
        jnp.bfloat16
    )
    attended = window_attention(normed_patches, vit_weight, vit_bias, window_ids)
    token_count = positions.shape[0]
    features = attended.reshape(token_count, -1)

    merger_weight = (merger_codes.astype(jnp.float32) * merger_scales.astype(jnp.float32)).astype(
        jnp.bfloat16
    )
    columns = merger_weight.shape[2]
    merger_weight = merger_weight.reshape(-1, columns)
    found, small = gather_features(features, jnp.concatenate([positions, segments]))
    all_positions = small[:, :token_count]
    all_segments = small[:, token_count:]
    early = max(1, groups_here - 1)
    gathered = [lax.all_gather(turned[:early], "ctx", axis=2, tiled=True)]
    sources = jnp.concatenate([source for source, _ in found])
    products = jnp.concatenate(
        [jnp.dot(rows, merger_weight, preferred_element_type=jnp.float32) for _, rows in found],
        axis=0,
    )
    part = columns // shares
    merged = summed_over_wt(
        turned_by_wt([products[:, k * part : (k + 1) * part] for k in range(shares)])
    ).astype(jnp.bfloat16)

    capacity = 2 * token_count // owners
    slots_each = owners * capacity
    target = all_positions // row_count
    item = jnp.arange(token_count, dtype=jnp.int32)
    before = (target[:, None, :] == target[:, :, None]) & (item[None, None, :] < item[None, :, None])
    ranks = jnp.sum(before.astype(jnp.int32), axis=2)
    slots = (
        target * slots_each + jnp.arange(owners, dtype=jnp.int32)[:, None] * capacity + ranks
    )
    slots_found = jnp.take(slots, sources, axis=0).reshape(-1)
    table = slots_found[None, :] == jnp.arange(owners * slots_each, dtype=jnp.int32)[:, None]
    mine = slots.reshape(1, -1) == me * slots_each + jnp.arange(slots_each, dtype=jnp.int32)[:, None]
    labels = jnp.sum(jnp.where(mine, all_positions.reshape(1, -1) + 1, 0), axis=1) - 1 - first
    place = labels[None, :] == jnp.arange(row_count, dtype=jnp.int32)[:, None]
    covered = jnp.any(place, axis=1)[:, None]
    table, place, covered = lax.optimization_barrier(
        (table.astype(jnp.bfloat16), place.astype(jnp.bfloat16), covered.astype(jnp.float32))
    )
    packed = jnp.dot(table, merged, preferred_element_type=jnp.float32).astype(jnp.bfloat16)
    arrived = lax.all_to_all(
        packed.reshape(owners, slots_each, part), "ctx", split_axis=0, concat_axis=0, tiled=True
    )
    if early < groups_here:
        late, arrived = lax.optimization_barrier((turned[early:], arrived))
        gathered.append(lax.all_gather(late, "ctx", axis=2, tiled=True))
    ours = turned_by_wt([block for block in arrived.reshape(shares, -1, slots_each, part)])
    held = [ours[0]] + [shifted(ours[k], "wt", k) for k in range(1, shares)]
    here = lax.axis_index("wt")
    whole_columns = jnp.concatenate(
        [lax.select_n((here - k) % shares, *held) for k in range(shares)], axis=2
    )
    flat = jnp.transpose(whole_columns, (1, 0, 2)).reshape(slots_each, -1)
    filled = jnp.dot(place, flat, preferred_element_type=jnp.float32)
    hidden = lax.optimization_barrier(
        jnp.where(covered > 0, (filled + merger_bias).astype(jnp.bfloat16), text_embed)
    )
    values = hidden.astype(jnp.float32)
    share = jnp.sum(values * values, axis=1)
    squares = share + sum(shifted(share, "wt", k) for k in range(1, shares))
    row_scale = lax.rsqrt(squares[:, None] / D + RMS_EPS)

    cosine, sine = rope_tables(first, row_count)
    sine = jnp.where(jnp.arange(HD) < HD // 2, -sine, sine)
    blocks = REACH + 1
    shards = me - jnp.arange(blocks, dtype=jnp.int32)
    key_segments = jnp.take(all_segments, jnp.maximum(shards, 0), axis=0)
    need = ((shards >= 0) & (key_segments[:, -1] >= segments[0])).astype(jnp.int32)
    query_segments = segments[None, :]
    key_segments = key_segments[:, :, None]
    ends = GROUP * HD
    full = ends + 2 * HD
    output = None
    for held, batch in zip(gathered, (range(early), range(early, groups_here))):
        finished = []
        for group in batch:
            if group == early:
                hidden, wide = lax.optimization_barrier((hidden, wide))
                arrivals = [wide] + [
                    passed_along(wide, "ctx", distance) for distance in range(1, blocks)
                ]
                waiting = (ready, jnp.stack(arrivals))
            elif group > 0:
                held, product = lax.optimization_barrier((held, product))
            columns_here = held[group - batch.start].reshape(shares * full, local_rows)
            product = lax.dot_general(
                hidden, columns_here, (((1,), (1,)), ((), ())), preferred_element_type=jnp.float32
            )
            if group == 0:
                product, row_scale = lax.optimization_barrier((product, row_scale))
            arrived = jnp.stack(
                [
                    shifted(product[:, k * full : (k + 1) * full].astype(jnp.bfloat16), "wt", k)
                    for k in range(1, shares)
                ]
            )
            finished.append(
                finish(
                    product,
                    arrived,
                    row_scale,
                    llm_bias[group][None, :],
                    cosine,
                    sine,
                    GROUP + 1,
                    [ends, 2 * HD],
                )
            )
        ready = [queries for queries, _ in finished]
        wide = jnp.concatenate([pair for _, pair in finished], axis=1)
    attending = [waiting] if early < groups_here else []
    arrivals = [wide] + [passed_along(wide, "ctx", distance) for distance in range(1, blocks)]
    attending.append((ready, jnp.stack(arrivals)))
    group = 0
    for ready, pieces in attending:
        for column, queries in enumerate(ready):
            output = attend(
                queries,
                pieces,
                column,
                query_segments,
                key_segments,
                need,
                group,
                groups_here,
                output,
            )
            group += 1
    return output


def solution(mesh):
    in_specs = (
        P("ctx", None),
        P(),
        P(None, None, "wt"),
        P("wt"),
        P(None, "wt"),
        P("ctx"),
        P(None, "wt", "ctx"),
        P(None, "wt", "ctx"),
        P("wt"),
        P("ctx"),
        P("ctx", "wt"),
        P("wt"),
        P("wt", None, "ctx"),
        P("wt", None, "ctx"),
        P("wt", None),
        P("ctx"),
    )
    out_specs = P("ctx", "wt")

    return jax.shard_map(
        on_device, mesh=mesh, in_specs=in_specs, out_specs=out_specs, check_vma=False
    )
```
